32 devices in a mesh: gx: 4 (over x, core), gy: 4 (over z), gz: 2 (over y).
Axes of the slice: x: 2, y: 2, z: 4, core: 2. Of those that a mesh axis runs over, the one named last changes fastest.
Arguments:
- right_side: float32 [16, 16, 8, 4, 256], P('gx', 'gy', 'gz'), may hold values from -80 to 80
- bond_blocks: float32 [13, 4, 4, 16, 16, 8], P(None, None, None, 'gx', 'gy', 'gz'), may hold values from -0.012 to 0.012
- bond_open: int32 [13, 16, 16, 8], P(None, 'gx', 'gy', 'gz'), may hold values 0 or 1
- onsite_blocks: float32 [4, 4, 16, 16, 8], P(None, None, 'gx', 'gy', 'gz'), may hold values from -0.012 to 0.012
- orbital_levels: float32 [4, 16, 16, 8], P(None, 'gx', 'gy', 'gz'), may hold values from 1.3 to 2.6
- column_shift: float32 [256], replicated, may hold values from 0.05 to 1
Outputs:
- solution: float32 [16, 16, 8, 4, 256], P('gx', 'gy', 'gz')
- residual: float32 [16, 16, 8, 4, 256], P('gx', 'gy', 'gz')
The draws below stay inside these ranges and needn't reach their ends.
All inputs are finite; a program needn't handle non-finite values. No bound on the sum of `bond_open` on one device may be relied on, other than what follows from the above.
Results may differ from the reference program's by a relative error of at most 0.0003.
Values sent between devices are 32-bit elements; how exact they have to be, the bound alone decides.
A program may use at most 192 MiB of HBM per device.

```python
import math
import jax
import jax.numpy as jnp
from jax import lax

ORB = 4
COLS = 256
BONDS = 13
ITERS = 3
NX = 16
NY = 16
NZ = 8


def draw_right_side(key, part):
    subkeys = jax.random.split(key, 3)
    full_shape = (NX, NY, NZ, ORB, COLS)
    along_x = jnp.arange(NX, dtype=jnp.float32) / NX
    along_y = jnp.arange(NY, dtype=jnp.float32) / NY
    along_z = jnp.arange(NZ, dtype=jnp.float32) / NZ
    position_ramp = jnp.exp(0.37 * (along_x[:, None, None] + along_y[None, :, None] + along_z[None, None, :]))
    atom_scale = jnp.exp(jax.random.uniform(subkeys[1], (NX, NY, NZ, ORB, 1), jnp.float32, math.log(0.3), math.log(3.0)))
    values = jnp.clip(jax.random.normal(subkeys[0], full_shape, jnp.float32), -4.0, 4.0)
    column_scale = jnp.exp(jax.random.uniform(subkeys[2], (COLS,), jnp.float32, math.log(0.5), math.log(5.0)))
    return (0.3 * values * atom_scale * column_scale * position_ramp[:, :, :, None, None]).astype(jnp.float32)


def set_ends(array, rng, least, largest):
    shape = array.shape
    place = [jax.random.randint(jax.random.fold_in(rng, axis), (), 0, shape[axis]) for axis in range(len(shape))]
    array = array.at[tuple(place)].set(least)
    longest = shape.index(max(shape))
    place[longest] = (place[longest] + 1) % shape[longest]
    return array.at[tuple(place)].set(largest)


def level_of(key, extent, pieces, smallest, high):
    factor_of, own = 1.0, jax.random.fold_in(key, 6)
    for axis_at, shards_of in pieces:
        steps = jnp.exp(jax.random.uniform(jax.random.fold_in(own, axis_at), (shards_of,), jnp.float32, smallest / len(pieces), high / len(pieces)))
        factor_of = factor_of * jnp.repeat(steps, extent[axis_at] // shards_of).reshape([-1 if axis == axis_at else 1 for axis in range(len(extent))])
    return factor_of


def setup_inputs(seed: int = 0) -> dict:
    keys = jax.random.split(jax.random.key(seed), 7)
    return {
        "right_side": draw_right_side(jax.random.fold_in(keys[6], 71), 0),
        "bond_blocks": jnp.clip(jax.random.uniform(keys[1], (BONDS, ORB, ORB, NX, NY, NZ), jnp.float32, -0.012, 0.012) * level_of(keys[1], (BONDS, ORB, ORB, NX, NY, NZ), ((3, 4), (4, 4), (5, 2)), -0.4, 0.0), -0.012, 0.012),
        "bond_open": set_ends((jax.random.randint(keys[2], (BONDS, NX, NY, NZ), 0, 4) < 3).astype(jnp.int32), jax.random.fold_in(keys[2], 1), 0, 1),
        "onsite_blocks": jnp.clip(jax.random.uniform(keys[3], (ORB, ORB, NX, NY, NZ), jnp.float32, -0.012, 0.012) * level_of(keys[3], (ORB, ORB, NX, NY, NZ), ((2, 4), (3, 4), (4, 2)), -0.4, 0.0), -0.012, 0.012),
        "orbital_levels": jnp.clip(jnp.exp(math.log(2.6) - 0.6931472 * jax.random.uniform(keys[4], (ORB, NX, NY, NZ), jnp.float32) ** level_of(keys[4], (ORB, NX, NY, NZ), ((1, 4), (2, 4), (3, 2)), -0.2, 0.2)), 1.3, 2.6),
        "column_shift": jnp.clip(jnp.exp(jax.random.uniform(keys[5], (COLS,), jnp.float32, math.log(0.05), math.log(1.0))), 0.05, 1.0),
    }


half_offsets = [(first, second, third) for first in (-1, 0, 1) for second in (-1, 0, 1) for third in (-1, 0, 1) if (first, second, third) > (0, 0, 0)]


def hop(blocks, vector):
    return jnp.einsum('ijxyz,xyzjc->xyzic', blocks.astype(jnp.float32), vector.astype(jnp.float32), precision=lax.Precision.HIGHEST)


def operate(vector, coupled, onsite_sym, atom_levels, column_shift):
    result = hop(onsite_sym, vector) + (atom_levels[..., None] + column_shift) * vector
    for bond_index, offset in enumerate(half_offsets):
        ahead = jnp.roll(vector, (-offset[0], -offset[1], -offset[2]), axis=(0, 1, 2))
        behind = jnp.roll(vector, offset, axis=(0, 1, 2))
        mirrored = jnp.roll(coupled[bond_index], offset, axis=(2, 3, 4))
        result = result + hop(coupled[bond_index], ahead) + hop(jnp.swapaxes(mirrored, 0, 1), behind)
    return result


def reference(right_side, bond_blocks, bond_open, onsite_blocks, orbital_levels, column_shift):
    coupled = bond_blocks * bond_open[:, None, None].astype(jnp.float32)
    onsite_sym = 0.5 * (onsite_blocks + jnp.swapaxes(onsite_blocks, 0, 1))
    atom_levels = jnp.transpose(orbital_levels, (1, 2, 3, 0))
    solution = jnp.zeros_like(right_side)
    residual = right_side
    direction = right_side
    norm_now = jnp.sum(residual * residual, axis=(0, 1, 2, 3))
    for iteration in range(ITERS):
        image = operate(direction, coupled, onsite_sym, atom_levels, column_shift)
        alpha = norm_now / jnp.sum(direction * image, axis=(0, 1, 2, 3))
        solution = solution + alpha * direction
        residual = residual - alpha * image
        norm_next = jnp.sum(residual * residual, axis=(0, 1, 2, 3))
        direction = residual + (norm_next / norm_now) * direction
        norm_now = norm_next
    return (solution, residual)
```

```python
import functools
import itertools

import jax
import jax.numpy as jnp
import numpy as np
from jax import lax
from jax.experimental import pallas as pl
from jax.experimental.pallas import tpu as pltpu
from jax.sharding import PartitionSpec as P

ITERS = 3
LANES = 128
HALF = 64
ROWS = 8
AXES = ("gx", "gy", "gz")
MESH = pl.DeviceIdType.MESH

half_offsets = [o for o in itertools.product((-1, 0, 1), repeat=3) if o > (0, 0, 0)]
directions = [d for d in itertools.product((-1, 0, 1), repeat=3) if d != (0, 0, 0)]


def up(value, step):
    return -(-value // step) * step


class Plan:
    def __init__(self, block, orbitals, peers_along):
        self.block, self.orb = block, orbitals
        self.own = block[0] * block[1] * block[2] * orbitals
        self.base = 4 * max(block) + 8
        codes = [self.code(p) for p in itertools.product(*map(range, block)) for _ in range(orbitals)]
        self.regions, at = [], 0
        for d in directions:
            here = [{0: range(n), 1: [n], -1: [-1]}[s] for s, n in zip(d, block)]
            there = [{0: range(n), 1: [0], -1: [n - 1]}[s] for s, n in zip(d, block)]
            positions = list(itertools.product(*here))
            codes += [self.code(p) for p in positions for _ in range(orbitals)]
            pieces = []
            for slot, p in enumerate(itertools.product(*there)):
                row = ((p[0] * block[1] + p[1]) * block[2] + p[2]) * orbitals
                target = at + slot * orbitals
                if pieces and pieces[-1][0] + pieces[-1][2] == row:
                    pieces[-1][2] += orbitals
                else:
                    pieces.append([row, target, orbitals])
            rows = len(positions) * orbitals
            size = up(rows, 8)
            codes += [10**6] * (size - rows)
            self.regions.append((d, at, rows, size, pieces))
            at += size
        self.halo = at
        self.ext = up(self.own + at, LANES)
        self.halo_all = self.ext - self.own
        codes += [10**6] * (self.ext - len(codes))
        self.codes = np.array(codes, np.float32)
        nx, ny, nz = peers_along
        self.peers_along = peers_along
        self.first = [(a, 0, c) for a in range(nx) for c in range(nz) if (a, c) != (0, 0)]
        self.second = [(0, b, 0) for b in range(1, ny)]
        greet = {tuple(s % n for s, n in zip(d, peers_along)) for d in directions}
        self.greet = sorted(greet | set(self.first) | set(self.second))

    def code(self, position):
        return (position[0] * self.base + position[1]) * self.base + position[2]


def kernel(plan, rs_ref, w_ref, shift_ref, code_ref, spread_ref, sol_ref, res_ref,
           send0, recv0, sends, recvs, ext, along, a_hi, a_lo, part1, got1, part2, got2,
           hs_sem, hr_sem, s1_sem, r1_sem, s2_sem, r2_sem):
    cols = rs_ref.shape[1]
    own, orb = plan.own, plan.orb
    halo, halo_all, full = plan.halo, plan.halo_all, plan.ext
    bonds = len(half_offsets)

    def at(relative):
        return tuple(
            lax.rem(lax.axis_index(name) + (s % n), n)
            for name, s, n in zip(AXES, relative, plan.peers_along)
        )

    barrier = pltpu.get_barrier_semaphore()
    for relative in plan.greet:
        pl.semaphore_signal(barrier, inc=1, device_id=at(relative), device_id_type=MESH)

    def pack(value, send_ref, lane):
        width = value.shape[1]
        for d, start, rows, size, pieces in plan.regions:
            parts = [value[source:source + count, :] for source, target, count in pieces]
            if size > rows:
                parts.append(jnp.zeros((size - rows, width), jnp.float32))
            whole = parts[0] if len(parts) == 1 else jnp.concatenate(parts, axis=0)
            send_ref[start:start + size, lane:lane + width] = whole

    pack(rs_ref[...], send0, 0)
    pack(w_ref[...], send0, cols)
    pl.semaphore_wait(barrier, len(plan.greet))

    def halo_copies(turn, source, target):
        copies = []
        for m, (d, start, rows, size, pieces) in enumerate(plan.regions):
            copies.append(pltpu.make_async_remote_copy(
                src_ref=source.at[pl.ds(start, size)],
                dst_ref=target.at[pl.ds(start, size)],
                send_sem=hs_sem.at[turn, m],
                recv_sem=hr_sem.at[turn, m],
                device_id=at(tuple(-s for s in d)),
                device_id_type=MESH,
            ))
        return copies

    flight = halo_copies(0, send0, recv0)
    for copy in flight:
        copy.start()

    code_lane = code_ref[...][0:1, :]
    code_row = jnp.transpose(jnp.broadcast_to(code_lane, (LANES, full)))[:, 0:1]
    steps = [float(plan.code(o)) for o in half_offsets]
    lane_of = lax.broadcasted_iota(jnp.int32, (LANES, LANES), 1)

    def spread(rows_of_w):
        high = rows_of_w.astype(jnp.bfloat16).astype(jnp.float32)
        both = jnp.where(lane_of < HALF, high, rows_of_w - high).astype(jnp.bfloat16)
        return jnp.dot(both, spread_ref[...], preferred_element_type=jnp.float32)

    def placed(tiles, row_codes, lane_codes, sign, count):
        width = lane_codes.shape[1]
        blocks = []
        for g in range(0, width, LANES):
            gap = (lane_codes[:, g:g + LANES] - row_codes) * sign
            total = jnp.zeros((LANES, LANES), jnp.float32)
            for k in range(count):
                step = steps[k] if k < bonds else 0.0
                total = jnp.where(gap == step, tiles[:, k * LANES:(k + 1) * LANES], total)
            blocks.append(total)
        return jnp.concatenate(blocks, axis=1)

    ext[0:own, :] = rs_ref[...]
    forward = []
    backward = []
    for b in range(0, own, LANES):
        tiles = spread(w_ref[b:b + LANES, :])
        forward.append(placed(tiles, code_row[b:b + LANES], code_lane, 1.0, bonds + 1))
        backward.append(placed(tiles, code_row[b:b + LANES], code_lane[:, 0:own], 1.0, bonds))
    for copy in flight:
        copy.wait_recv()
    ext[own:own + halo, :] = recv0[0:halo, 0:cols]
    if own + halo < full:
        ext[own + halo:full, :] = jnp.zeros((full - own - halo, cols), jnp.float32)
        recv0[halo:halo_all, :] = jnp.zeros((halo_all - halo, cols + LANES), jnp.float32)
    for b in range(0, halo_all, LANES):
        tiles = spread(recv0[b:b + LANES, cols:cols + LANES])
        rows = code_row[own + b:own + b + LANES]
        backward.append(placed(tiles, rows, code_lane[:, 0:own], 1.0, bonds))
    for b in range(0, own, LANES):
        for g in range(0, full, LANES):
            block = forward[b // LANES][:, g:g + LANES] + jnp.transpose(backward[g // LANES][:, b:b + LANES])
            high = block.astype(jnp.bfloat16)
            a_hi[b:b + LANES, g:g + LANES] = high
            a_lo[b:b + LANES, g:g + LANES] = (block - high.astype(jnp.float32)).astype(jnp.bfloat16)

    diagonal = w_ref[...][:, (bonds + 1) * orb:(bonds + 1) * orb + 1] + shift_ref[...]

    def operate():
        vector = ext[...]
        high = vector.astype(jnp.bfloat16)
        low = (vector - high.astype(jnp.float32)).astype(jnp.bfloat16)
        total = jnp.dot(a_hi[...], low, preferred_element_type=jnp.float32)
        total = total + jnp.dot(a_lo[...], high, preferred_element_type=jnp.float32)
        total = total + jnp.dot(a_hi[...], high, preferred_element_type=jnp.float32)
        return total + diagonal * ext[0:own, :]

    pending = list(flight)

    def group(turn, members, source, target, send_sem, recv_sem):
        copies = []
        for m, relative in enumerate(members):
            copies.append(pltpu.make_async_remote_copy(
                src_ref=source.at[turn],
                dst_ref=target.at[turn, m],
                send_sem=send_sem.at[turn, m],
                recv_sem=recv_sem.at[turn, m],
                device_id=at(relative),
                device_id_type=MESH,
            ))
        for copy in copies:
            copy.start()
        pending.extend(copies)
        return copies

    for turn in range(ITERS):
        image = operate()
        mine = ext[0:own, :]
        part1[turn] = jnp.concatenate([
            jnp.sum(mine * mine, axis=0, keepdims=True),
            jnp.sum(mine * image, axis=0, keepdims=True),
            jnp.zeros((ROWS - 2, cols), jnp.float32),
        ], axis=0)
        sums = group(turn, plan.first, part1, got1, s1_sem, r1_sem)
        last = turn + 1 == ITERS
        if turn == 0:
            along[0:own, :] = image
        else:
            res_ref[...] = image
        if not last:
            pack(image, sends.at[turn], 0)
            flight = halo_copies(turn + 1, sends.at[turn], recvs.at[turn])
            for copy in flight:
                copy.start()
            pending.extend(flight)
        total = part1[turn]
        for m, copy in enumerate(sums):
            copy.wait_recv()
            total = total + got1[turn, m]
        part2[turn] = total
        sums = group(turn, plan.second, part2, got2, s2_sem, r2_sem)
        for m, copy in enumerate(sums):
            copy.wait_recv()
            total = total + got2[turn, m]
        norm, product = total[0:1], total[1:2]
        if turn == 0:
            alpha = norm / product
            direction = mine
            sol_ref[...] = alpha * mine
        else:
            ratio = norm / norm_before
            alpha = norm / (product - ratio * norm / alpha)
            direction = mine + ratio * direction
            sol_ref[...] = sol_ref[...] + alpha * direction
            along[0:own, :] = res_ref[...] + ratio * along[0:own, :]
        norm_before = norm
        if last:
            res_ref[...] = mine - alpha * along[0:own, :]
        else:
            ext[0:own, :] = mine - alpha * along[0:own, :]
            for copy in flight:
                copy.wait_recv()
            edge = recvs[turn, 0:halo, :]
            if turn > 0:
                edge = edge + ratio * along[own:own + halo, :]
            along[own:own + halo, :] = edge
            ext[own:own + halo, :] = ext[own:own + halo, :] - alpha * edge
    for copy in pending:
        copy.wait_send()


def per_device(peers_along, right_side, bond_blocks, bond_open, onsite_blocks, orbital_levels, column_shift):
    block, orb, cols = right_side.shape[:3], right_side.shape[3], right_side.shape[4]
    plan = Plan(block, orb, peers_along)
    own, bonds = plan.own, len(half_offsets)
    coupled = bond_blocks * bond_open[:, None, None].astype(jnp.float32)
    onsite_sym = 0.5 * (onsite_blocks + jnp.swapaxes(onsite_blocks, 0, 1))
    atoms = own // orb
    lines = jnp.concatenate([coupled, onsite_sym[None]], axis=0).reshape(bonds + 1, orb, orb, atoms)
    lines = jnp.transpose(lines, (3, 1, 0, 2)).reshape(own, (bonds + 1) * orb)
    levels = jnp.transpose(orbital_levels.reshape(orb, atoms)).reshape(own, 1)
    lines = jnp.concatenate([lines, levels, jnp.zeros((own, HALF - lines.shape[1] - 1), jnp.float32)], axis=1)
    lines = jnp.concatenate([lines, lines], axis=1)

    count = bonds + 1
    spread = np.zeros((2, HALF, count, LANES), np.float32)
    for k in range(count):
        for t in range(LANES):
            spread[:, k * orb + t % orb, k, t] = 1.0
    spread = jnp.asarray(spread.reshape(LANES, count * LANES), jnp.bfloat16)
    code = jnp.asarray(np.tile(plan.codes[None], (8, 1)))
    f32, bf16 = jnp.float32, jnp.bfloat16
    n1, n2, messages = len(plan.first), len(plan.second), len(directions)
    dma = pltpu.SemaphoreType.DMA
    vmem = pl.BlockSpec(memory_space=pltpu.VMEM)
    solved, left = pl.pallas_call(
        functools.partial(kernel, plan),
        out_shape=(jax.ShapeDtypeStruct((own, cols), f32),) * 2,
        in_specs=[vmem] * 5,
        out_specs=(vmem, vmem),
        scratch_shapes=[
            pltpu.VMEM((plan.halo_all + ROWS, cols + LANES), f32),
            pltpu.VMEM((plan.halo_all, cols + LANES), f32),
            pltpu.VMEM((ITERS - 1, plan.halo_all + ROWS, cols), f32),
            pltpu.VMEM((ITERS - 1, plan.halo_all, cols), f32),
            pltpu.VMEM((plan.ext, cols), f32),
            pltpu.VMEM((plan.ext, cols), f32),
            pltpu.VMEM((own, plan.ext), bf16),
            pltpu.VMEM((own, plan.ext), bf16),
            pltpu.VMEM((ITERS, ROWS, cols), f32),
            pltpu.VMEM((ITERS, n1, ROWS, cols), f32),
            pltpu.VMEM((ITERS, ROWS, cols), f32),
            pltpu.VMEM((ITERS, n2, ROWS, cols), f32),
            dma((ITERS, messages)), dma((ITERS, messages)),
            dma((ITERS, n1)), dma((ITERS, n1)),
            dma((ITERS, n2)), dma((ITERS, n2)),
        ],
        compiler_params=pltpu.CompilerParams(
            collective_id=0, has_side_effects=True, vmem_limit_bytes=60 * 1024 * 1024
        ),
    )(right_side.reshape(own, cols), lines, column_shift[None], code, spread)
    return solved.reshape(right_side.shape), left.reshape(right_side.shape)


def solution(mesh):
    field = P("gx", "gy", "gz", None, None)
    placed = (
        field,
        P(None, None, None, "gx", "gy", "gz"),
        P(None, "gx", "gy", "gz"),
        P(None, None, "gx", "gy", "gz"),
        P(None, "gx", "gy", "gz"),
        P(),
    )
    return jax.shard_map(
        functools.partial(per_device, tuple(mesh.shape[name] for name in AXES)),
        mesh=mesh,
        in_specs=placed,
        out_specs=(field, field),
        check_vma=False,
    )
```
